32 devices in a mesh: rows: 32 (over z, y, x, core).
Axes of the slice: x: 2, y: 2, z: 4, core: 2. Of those that a mesh axis runs over, the one named last changes fastest.
Arguments:
- blocks: float32 [512, 4, 256, 256], P('rows'), may hold values from -0.125 to 0.125
- block_cols: int32 [512, 4], P('rows'), may hold values from 0 to 511, as said below
- live_counts: int32 [512], P('rows'), may hold values from 1 to 4, as said below
- onsite_energy: float32 [131072], P('rows'), may hold values from -2 to 2
- precond: float32 [512, 256, 256], P('rows')
- vectors: float32 [32, 131072], P(None, 'rows'), may hold values from -6 to 6
- prev_vectors: float32 [32, 131072], P(None, 'rows'), may hold values from -6 to 6
- prev_image: float32 [32, 131072], P(None, 'rows'), may hold values from -6 to 6
Outputs:
- correction: float32 [32, 131072], P(None, 'rows')
- reduced: float32 [96, 96], replicated
The draws below stay inside these ranges and needn't reach their ends.
Inputs may be any that keep to these rules, and one draw needn't show every extreme that they name: block_cols[b, s] = (b + o) mod 512, with the offsets o of one block-row distinct and within 0 to 4; every slot holds a valid block-column. Slots s < live_counts[b] are live, the rest are ignored; some block-row has 4 live slots in every draw.
All inputs are finite; a program needn't handle non-finite values.
Results may differ from the reference program's by a relative error of at most 0.00026.
Values sent between devices are 32-bit elements; how exact they have to be, the bound alone decides.
A program may use at most 128 MiB of HBM per device.

```python
import jax
import jax.numpy as jnp
from jax import lax

BS = 256
K = 32
BR_DEV = 16
HB = 4
MAXB = 4
ITERS = 3
NBR = 512
NROWS = 131072
BASIS = 96


def draw_block_cols(key, part):
    scores = jax.random.randint(key, (NBR, HB + 1), 0, 1 << 20) * (HB + 1) + jnp.arange(HB + 1, dtype=jnp.int32)[None, :]
    offsets = jnp.argsort(scores, axis=1)[:, :MAXB].astype(jnp.int32)
    return ((jnp.arange(NBR, dtype=jnp.int32)[:, None] + offsets) % NBR).astype(jnp.int32)


def draw_live_counts(key, part):
    first_key = jax.random.fold_in(key, 11)
    second_key = jax.random.fold_in(key, 23)
    third_key = jax.random.fold_in(key, 37)
    shifts = jax.random.randint(first_key, (NBR // BR_DEV,), 0, 3)
    ceiling = jnp.maximum(jnp.right_shift(jnp.full((NBR // BR_DEV,), MAXB, jnp.int32), shifts), 1)
    ceiling_rows = jnp.repeat(ceiling, BR_DEV)
    uniform_ints = jax.random.randint(second_key, (NBR,), 0, 1024)
    counts = 1 + uniform_ints * ceiling_rows // 1024
    position = jax.random.randint(third_key, (), 0, NBR)
    return counts.at[position].set(MAXB).astype(jnp.int32)


def draw_precond(key, part):
    noise = jax.random.normal(key, (NBR, BS, BS), jnp.float32)
    return jnp.eye(BS, dtype=jnp.float32)[None, :, :] + 0.5 * noise / jnp.sqrt(jnp.float32(BS))


def level_of(own_key, extent, shards, least, largest):
    def one(dim, shards_of):
        steps = jax.random.uniform(jax.random.fold_in(jax.random.fold_in(own_key, 6), dim), (shards_of,), jnp.float32, least / len(shards), largest / len(shards))
        return jnp.repeat(jnp.exp(steps), extent[dim] // shards_of).reshape((-1,) + (1,) * (len(extent) - dim - 1))

    loudness = one(*shards[0])
    for cut in shards[1:]:
        loudness = loudness * one(*cut)
    return loudness


def normal_values(key, extent, scale, reach, split=(), kind=jnp.bfloat16):
    drawn = scale * jax.random.normal(key, extent, jnp.float32)
    if split:
        drawn = drawn * level_of(key, extent, split, -0.22, 0.18)
    return jnp.clip(drawn, -reach, reach).astype(kind)


def setup_inputs(seed: int = 0) -> dict:
    seeds = jax.random.split(jax.random.key(seed), 9)
    return {
        "blocks": normal_values(seeds[0], (NBR, MAXB, BS, BS), (2 * MAXB * BS) ** -0.5, 0.125, ((0, 32),), jnp.float32),
        "block_cols": draw_block_cols(jax.random.fold_in(seeds[8], 71), 0),
        "live_counts": draw_live_counts(jax.random.fold_in(seeds[8], 71), 0),
        "onsite_energy": jnp.clip(jax.random.uniform(seeds[3], (NROWS,), jnp.float32, -2.0, 2.0) * level_of(seeds[3], (NROWS,), ((0, 32),), -0.4, 0.0), -2.0, 2.0),
        "precond": draw_precond(jax.random.fold_in(seeds[8], 71), 0),
        "vectors": normal_values(seeds[5], (K, NROWS), 1.0, 6.0, ((1, 32),), jnp.float32),
        "prev_vectors": normal_values(seeds[6], (K, NROWS), 1.0, 6.0, ((1, 32),), jnp.float32),
        "prev_image": normal_values(seeds[7], (K, NROWS), 1.0, 6.0, ((1, 32),), jnp.float32),
    }


def operate(field, blocks, block_cols, live_mask, onsite_energy):
    vec_count = field.shape[0]
    source = field.reshape(vec_count, NBR, BS)
    picked = source[:, block_cols] * live_mask[None, :, :, None]
    forward_part = jnp.einsum('bsij,kbsj->kbi', blocks, picked, precision=lax.Precision.HIGHEST)
    moved = jnp.einsum('kbi,bsij->kbsj', source, blocks, precision=lax.Precision.HIGHEST) * live_mask[None, :, :, None]
    spread = jnp.zeros_like(source).at[:, block_cols].add(moved)
    return onsite_energy[None, :] * field + (forward_part + spread).reshape(vec_count, -1)

def reference(blocks, block_cols, live_counts, onsite_energy, precond, vectors, prev_vectors, prev_image):
    live_mask = (jnp.arange(MAXB, dtype=jnp.int32)[None, :] < live_counts[:, None]).astype(jnp.float32)
    image = operate(vectors, blocks, block_cols, live_mask, onsite_energy)
    quotient = jnp.sum(vectors * image, axis=1) / jnp.sum(vectors * vectors, axis=1)
    remainder = -(image - quotient[:, None] * vectors)
    correction = jnp.zeros_like(vectors)
    hcorr = jnp.zeros_like(vectors)
    for iteration in range(ITERS):
        search = jnp.einsum('bij,kbj->kbi', precond, remainder.reshape(K, NBR, BS), precision=lax.Precision.HIGHEST).reshape(K, -1)
        applied = operate(search, blocks, block_cols, live_mask, onsite_energy) - quotient[:, None] * search
        step_size = jnp.sum(applied * remainder, axis=1) / (jnp.sum(applied * applied, axis=1) + 1.0)
        correction = correction + step_size[:, None] * search
        hcorr = hcorr + step_size[:, None] * (applied + quotient[:, None] * search)
        remainder = remainder - step_size[:, None] * applied
    basis = jnp.concatenate([vectors, prev_vectors, correction], axis=0)
    himage = jnp.concatenate([image, prev_image, hcorr], axis=0)
    gram_matrix = jnp.dot(basis, basis.T, precision=lax.Precision.HIGHEST) + jnp.eye(BASIS, dtype=jnp.float32)
    projected = jnp.dot(basis, himage.T, precision=lax.Precision.HIGHEST)
    factor = jnp.linalg.cholesky(gram_matrix)
    half_way = jax.scipy.linalg.solve_triangular(factor, projected, lower=True)
    reduced = jax.scipy.linalg.solve_triangular(factor, half_way.T, lower=True).T
    return (correction, reduced)
```

```python
import functools

import jax
import jax.numpy as jnp
from jax import lax
from jax.experimental import pallas as pl
from jax.experimental.pallas import tpu as pltpu
from jax.sharding import PartitionSpec as P

HB = 4
ITERS = 3
MESH = pl.DeviceIdType.MESH
F32 = jnp.float32
BF16 = jnp.bfloat16
NN = (((1,), (0,)), ((), ()))
NT = (((1,), (1,)), ((), ()))


def split(x):
    high = x.astype(BF16)
    low = (x - high.astype(F32)).astype(BF16)
    return high, low


def dot(a, b, dims):
    return lax.dot_general(a, b, dims, preferred_element_type=F32)


def dot3(pair, high, low, dims):
    rows = pair.shape[0] // 2
    both = dot(pair, high, dims)
    return both[:rows] + both[rows:] + dot(pair[:rows], low, dims)


def kernel(
    n, cols, counts, blocks, precond, onsite, vectors, prev_vectors, prev_image,
    correction, reduced,
    w_high, w_low, m_high, m_low, stage, pstage, field, pair, acc, image, rem, app, hcorr,
    halo_in, land_in, part, sums_in, gp, gp_in, gsum, gall, work,
    load_sem, pload_sem, halo_send, halo_recv, land_send, land_recv,
    sum_send, sum_recv, gp_send, gp_recv, ga_send, ga_recv,
):
    me = lax.axis_index("rows")
    right, left = lax.rem(me + 1, n), lax.rem(me + n - 1, n)
    br, slots, bs = blocks.shape[0], blocks.shape[1], blocks.shape[2]
    kv = vectors.shape[0]
    total = br * n
    first = br - HB

    def lanes(b):
        return pl.ds(pl.multiple_of(b * bs, bs), bs)

    def order(t):
        return lax.rem(t + first, br)

    def load(t):
        b = order(t)
        return pltpu.make_async_copy(blocks.at[b], stage.at[lax.rem(t, 3)], load_sem.at[lax.rem(t, 3)])

    def pload(b):
        return pltpu.make_async_copy(precond.at[b], pstage.at[lax.rem(b, 2)], pload_sem.at[lax.rem(b, 2)])

    load(0).start()
    load(1).start()
    load(2).start()
    pload(0).start()
    pload(1).start()

    barrier = pltpu.get_barrier_semaphore()

    def greet(d, _):
        pl.semaphore_signal(barrier, inc=1, device_id=(lax.rem(me + d, n),), device_id_type=MESH)
        return 0

    lax.fori_loop(1, n, greet, 0)

    def take_vectors(b, _):
        x = vectors[:, lanes(b)]
        field[b] = x
        high, low = split(x)
        pair[b, :kv] = high
        pair[b, kv:] = low
        return 0

    lax.fori_loop(0, br, take_vectors, 0)
    pair[br + HB] = jnp.zeros((2 * kv, bs), BF16)
    pl.semaphore_wait(barrier, n - 1)

    def offset(b, s):
        return lax.rem(cols[b, s] - (me * br + b) + total, total)

    def spread(b):
        moved = dot3(pair[b], w_high[b], w_low[b], NN)
        parts = [moved[:, s * bs:(s + 1) * bs] for s in range(slots)]
        offs = [jnp.where(s < counts[b], offset(b, s), HB + 1) for s in range(slots)]
        for k in range(HB + 1):
            got = acc[b + k]
            for s in range(slots):
                got = got + jnp.where(offs[s] == k, 1.0, 0.0).astype(F32) * parts[s]
            acc[b + k] = got

    def forward(b):
        picks = []
        for s in range(slots):
            at = jnp.where(s < counts[b], b + offset(b, s), br + HB)
            picks.append(pair[at])
        wide = jnp.concatenate(picks, axis=1)
        acc[b] = acc[b] + dot3(wide, w_high[b], w_low[b], NT)

    def take_tiles(t):
        load(t).wait()
        b = order(t)
        for s in range(slots):
            high, low = split(stage[lax.rem(t, 3), s])
            w_high[b, :, s * bs:(s + 1) * bs] = high
            w_low[b, :, s * bs:(s + 1) * bs] = low

        @pl.when(t + 3 < br)
        def _():
            load(t + 3).start()

    def operate(k, loading):
        halo = pltpu.make_async_remote_copy(
            src_ref=field.at[pl.ds(0, HB)], dst_ref=halo_in.at[k],
            send_sem=halo_send.at[k], recv_sem=halo_recv.at[k],
            device_id=(left,), device_id_type=MESH)
        halo.start()

        def clear(b, _):
            acc[b] = jnp.zeros((kv, bs), F32)
            return 0

        lax.fori_loop(0, br + HB, clear, 0)

        def late(t, _):
            if loading:
                take_tiles(t)
            spread(first + t)
            return 0

        lax.fori_loop(0, HB, late, 0)
        land = pltpu.make_async_remote_copy(
            src_ref=acc.at[pl.ds(br, HB)], dst_ref=land_in.at[k],
            send_sem=land_send.at[k], recv_sem=land_recv.at[k],
            device_id=(right,), device_id_type=MESH)
        land.start()

        def main(b, _):
            if loading:
                take_tiles(b + HB)
            spread(b)
            if not loading:
                forward(b)
            return 0

        lax.fori_loop(0, first, main, 0)
        if loading:
            def again(b, _):
                forward(b)
                return 0

            lax.fori_loop(0, first, again, 0)
        halo.wait_recv()

        def take_halo(i, _):
            high, low = split(halo_in[k, i])
            pair[br + i, :kv] = high
            pair[br + i, kv:] = low
            return 0

        lax.fori_loop(0, HB, take_halo, 0)

        def tail(b, _):
            forward(b)
            return 0

        lax.fori_loop(first, br, tail, 0)
        land.wait_recv()

        def take_land(i, _):
            acc[i] = acc[i] + land_in[k, i]
            return 0

        lax.fori_loop(0, HB, take_land, 0)
        halo.wait_send()
        land.wait_send()

    def all_sum(k, one, two):
        folded = jnp.concatenate([one, two], axis=0)
        folded = folded[:, :128] + folded[:, 128:]
        wide = jnp.broadcast_to(jnp.sum(folded, axis=1, keepdims=True), (2 * kv, 128))
        wide = jnp.concatenate([wide, jnp.zeros((128 - 2 * kv, 128), F32)], axis=0)
        mine = wide.T[:8]
        part[k] = mine
        sums_in[k, me] = mine

        def copy(d):
            return pltpu.make_async_remote_copy(
                src_ref=part.at[k], dst_ref=sums_in.at[k, me],
                send_sem=sum_send.at[k, d], recv_sem=sum_recv.at[k, me],
                device_id=(lax.rem(me + d, n),), device_id_type=MESH)

        def send(d, _):
            copy(d).start()
            return 0

        lax.fori_loop(1, n, send, 0)

        def arrive(d, _):
            who = lax.rem(me + d, n)
            pltpu.make_async_remote_copy(
                src_ref=part.at[k], dst_ref=sums_in.at[k, who],
                send_sem=sum_send.at[k, d], recv_sem=sum_recv.at[k, who],
                device_id=(who,), device_id_type=MESH).wait_recv()
            return 0

        lax.fori_loop(1, n, arrive, 0)

        def add(i, so_far):
            return so_far + sums_in[k, i]

        whole = lax.fori_loop(0, n, add, jnp.zeros((8, 128), F32))

        def sent(d, _):
            copy(d).wait_send()
            return 0

        lax.fori_loop(1, n, sent, 0)
        column = jnp.broadcast_to(whole[0:1], (128, 128)).T
        column = jnp.concatenate([column, column], axis=1)
        return column[:kv], column[kv:2 * kv]

    zero = jnp.zeros((kv, bs), F32)
    operate(0, True)

    def rayleigh(b, sums):
        x = vectors[:, lanes(b)]
        y = acc[b] + onsite[:, lanes(b)] * x
        image[b] = y
        return sums[0] + x * y, sums[1] + x * x

    numerator, denominator = all_sum(0, *lax.fori_loop(0, br, rayleigh, (zero, zero)))
    quotient = numerator / denominator

    def take_precond(b, _):
        pload(b).wait()
        high, low = split(pstage[lax.rem(b, 2)])
        m_high[b] = high
        m_low[b] = low

        @pl.when(b + 2 < br)
        def _():
            pload(b + 2).start()
        rem[b] = quotient * vectors[:, lanes(b)] - image[b]
        correction[:, lanes(b)] = zero
        hcorr[b] = zero
        return 0

    lax.fori_loop(0, br, take_precond, 0)

    for it in range(ITERS):
        def search(b, _):
            high, low = split(rem[b])
            x = dot3(jnp.concatenate([high, low], axis=0), m_high[b], m_low[b], NT)
            field[b] = x
            high, low = split(x)
            pair[b, :kv] = high
            pair[b, kv:] = low
            return 0

        lax.fori_loop(0, br, search, 0)
        operate(it + 1, False)

        def apply(b, sums):
            y = acc[b] + (onsite[:, lanes(b)] - quotient) * field[b]
            app[b] = y
            return sums[0] + y * rem[b], sums[1] + y * y

        cross, own = all_sum(it + 1, *lax.fori_loop(0, br, apply, (zero, zero)))
        step = cross / (own + 1.0)

        def update(b, _):
            x, y = field[b], app[b]
            correction[:, lanes(b)] = correction[:, lanes(b)] + step * x
            hcorr[b] = hcorr[b] + step * (y + quotient * x)
            rem[b] = rem[b] - step * y
            return 0

        lax.fori_loop(0, br, update, 0)

    nb = 3 * kv

    def gram(b, so_far):
        basis = jnp.concatenate(
            [vectors[:, lanes(b)], prev_vectors[:, lanes(b)], correction[:, lanes(b)]], axis=0)
        other = jnp.concatenate([image[b], prev_image[:, lanes(b)], hcorr[b]], axis=0)
        bh, bl = split(basis)
        oh, ol = split(other)
        high = jnp.concatenate([bh, oh], axis=0)
        low = jnp.concatenate([bl, ol], axis=0)
        return so_far + dot(bh, high, NT) + dot(bl, high, NT) + dot(bh, low, NT)

    both = lax.fori_loop(0, br, gram, jnp.zeros((nb, 2 * nb), F32))
    pad = jnp.zeros((nb, 128 - nb), F32)
    sheet = jnp.concatenate(
        [jnp.concatenate([both[:, :nb], pad], axis=1), jnp.concatenate([both[:, nb:], pad], axis=1)],
        axis=0)
    chunks = 2 * nb // 8
    for c in range(chunks):
        gp[c] = sheet[c * 8:(c + 1) * 8]

    def scatter(d):
        to = lax.rem(me + d, n)
        return to, pltpu.make_async_remote_copy(
            src_ref=gp.at[jnp.minimum(to, chunks - 1)], dst_ref=gp_in.at[me],
            send_sem=gp_send.at[d], recv_sem=gp_recv.at[me],
            device_id=(to,), device_id_type=MESH)

    def scatter_send(d, _):
        to, copy = scatter(d)

        @pl.when(to < chunks)
        def _():
            copy.start()
        return 0

    lax.fori_loop(1, n, scatter_send, 0)

    def gather(d):
        to = lax.rem(me + d, n)
        return pltpu.make_async_remote_copy(
            src_ref=gsum, dst_ref=gall.at[me],
            send_sem=ga_send.at[d], recv_sem=ga_recv.at[me],
            device_id=(to,), device_id_type=MESH)

    @pl.when(me < chunks)
    def _():
        gp_in[me] = gp[me]

        def arrive(d, _):
            who = lax.rem(me + d, n)
            pltpu.make_async_remote_copy(
                src_ref=gsum, dst_ref=gp_in.at[who],
                send_sem=gp_send.at[d], recv_sem=gp_recv.at[who],
                device_id=(who,), device_id_type=MESH).wait_recv()
            return 0

        lax.fori_loop(1, n, arrive, 0)

        def add(i, so_far):
            return so_far + gp_in[i]

        mine = lax.fori_loop(0, n, add, jnp.zeros((8, 128), F32))
        gsum[...] = mine
        gall[me] = mine

        def send(d, _):
            gather(d).start()
            return 0

        lax.fori_loop(1, n, send, 0)

    def gathered(c, _):
        @pl.when(c != me)
        def _():
            pltpu.make_async_remote_copy(
                src_ref=gsum, dst_ref=gall.at[c],
                send_sem=ga_send.at[0], recv_sem=ga_recv.at[c],
                device_id=(right,), device_id_type=MESH).wait_recv()
        return 0

    lax.fori_loop(0, chunks, gathered, 0)

    def scatter_done(d, _):
        to, copy = scatter(d)

        @pl.when(to < chunks)
        def _():
            copy.wait_send()

        @pl.when(me < chunks)
        def _():
            gather(d).wait_send()
        return 0

    lax.fori_loop(1, n, scatter_done, 0)

    rows_at = lax.broadcasted_iota(jnp.int32, (nb, 128), 0)
    cols_at = lax.broadcasted_iota(jnp.int32, (nb, 128), 1)
    eye = jnp.where(rows_at == cols_at, 1.0, 0.0).astype(F32)
    half = chunks // 2
    g = jnp.concatenate([gall[c] for c in range(half)], axis=0)
    p = jnp.concatenate([gall[half + c] for c in range(half)], axis=0)
    work[:, 0:128] = g + eye
    work[:, 128:256] = p
    work[:, 256:384] = eye

    def eliminate(j, _):
        column = jnp.sum(jnp.where(cols_at == j, work[:, 0:128], 0.0), axis=1, keepdims=True)
        row = work[pl.ds(j, 1), :]
        pivot = jnp.sum(jnp.where(lax.broadcasted_iota(jnp.int32, (1, 128), 1) == j, row[:, :128], 0.0), axis=1, keepdims=True)
        root = 1.0 / jnp.sqrt(pivot)
        row = row * root
        below = jnp.where(rows_at[:, 0:1] > j, column * root, 0.0)
        work[...] = work[...] - below * row
        work[pl.ds(j, 1), :] = row
        return 0

    lax.fori_loop(0, nb, eliminate, 0)
    half_way = work[:, 128:256]
    inverse = work[:, 256:384]
    answer = lax.dot_general(
        half_way[:, :nb], inverse[:, :nb], NT, precision=lax.Precision.HIGHEST,
        preferred_element_type=F32)
    reduced[...] = answer


def local(blocks, block_cols, live_counts, onsite_energy, precond, vectors, prev_vectors, prev_image):
    n = lax.axis_size("rows")
    br, slots, bs, _ = blocks.shape
    kv, width = vectors.shape
    nb = 3 * kv
    vmem = pl.BlockSpec(memory_space=pltpu.VMEM)
    smem = pl.BlockSpec(memory_space=pltpu.SMEM)
    hbm = pl.BlockSpec(memory_space=pl.ANY)
    dma = pltpu.SemaphoreType.DMA
    rounds = ITERS + 1
    chunks = 2 * nb // 8
    return pl.pallas_call(
        functools.partial(kernel, n),
        out_shape=(
            jax.ShapeDtypeStruct((kv, width), F32),
            jax.ShapeDtypeStruct((nb, nb), F32),
        ),
        in_specs=[smem, smem, hbm, hbm, vmem, vmem, vmem, vmem],
        out_specs=(vmem, vmem),
        scratch_shapes=[
            pltpu.VMEM((br, bs, slots * bs), BF16),
            pltpu.VMEM((br, bs, slots * bs), BF16),
            pltpu.VMEM((br, bs, bs), BF16),
            pltpu.VMEM((br, bs, bs), BF16),
            pltpu.VMEM((3, slots, bs, bs), F32),
            pltpu.VMEM((2, bs, bs), F32),
            pltpu.VMEM((br, kv, bs), F32),
            pltpu.VMEM((br + HB + 1, 2 * kv, bs), BF16),
            pltpu.VMEM((br + HB, kv, bs), F32),
            pltpu.VMEM((br, kv, bs), F32),
            pltpu.VMEM((br, kv, bs), F32),
            pltpu.VMEM((br, kv, bs), F32),
            pltpu.VMEM((br, kv, bs), F32),
            pltpu.VMEM((rounds, HB, kv, bs), F32),
            pltpu.VMEM((rounds, HB, kv, bs), F32),
            pltpu.VMEM((rounds, 8, 128), F32),
            pltpu.VMEM((rounds, n, 8, 128), F32),
            pltpu.VMEM((chunks, 8, 128), F32),
            pltpu.VMEM((n, 8, 128), F32),
            pltpu.VMEM((8, 128), F32),
            pltpu.VMEM((chunks, 8, 128), F32),
            pltpu.VMEM((nb, 384), F32),
            dma((3,)),
            dma((2,)),
            dma((rounds,)),
            dma((rounds,)),
            dma((rounds,)),
            dma((rounds,)),
            dma((rounds, n)),
            dma((rounds, n)),
            dma((n,)),
            dma((n,)),
            dma((n,)),
            dma((n,)),
        ],
        compiler_params=pltpu.CompilerParams(
            collective_id=0, has_side_effects=True, vmem_limit_bytes=60 * 1024 * 1024
        ),
    )(block_cols, live_counts, blocks, precond, onsite_energy[None, :], vectors, prev_vectors, prev_image)


def solution(mesh):
    placed = (
        P("rows", None, None, None),
        P("rows", None),
        P("rows"),
        P("rows"),
        P("rows", None, None),
        P(None, "rows"),
        P(None, "rows"),
        P(None, "rows"),
    )
    return jax.shard_map(
        local, mesh=mesh, in_specs=placed, out_specs=(P(None, "rows"), P()), check_vma=False
    )
```

```python
import functools

import jax
import jax.numpy as jnp
from jax import lax
from jax.experimental import pallas as pl
from jax.experimental.pallas import tpu as pltpu
from jax.sharding import PartitionSpec as P

HB = 4
ITERS = 3
MESH = pl.DeviceIdType.MESH
F32 = jnp.float32
BF16 = jnp.bfloat16
NN = (((1,), (0,)), ((), ()))
NT = (((1,), (1,)), ((), ()))


def split(x):
    high = x.astype(BF16)
    low = (x - high.astype(F32)).astype(BF16)
    return high, low


def dot(a, b, dims):
    return lax.dot_general(a, b, dims, preferred_element_type=F32)


def dot3(pair, high, low, dims):
    rows = pair.shape[0] // 2
    both = dot(pair, high, dims)
    return both[:rows] + both[rows:] + dot(pair[:rows], low, dims)


def kernel(
    n, cols, counts, blocks, precond, onsite, vectors, prev_vectors, prev_image,
    correction, reduced,
    w_high, w_low, m_high, m_low, stage, pstage, field, pair, acc, image, rem, app, hcorr, srch,
    halo_in, land_in, part, sums_in, gp, gp_in, gsum, gall, work,
    load_sem, pload_sem, halo_send, halo_recv, land_send, land_recv,
    sum_send, sum_recv, gp_send, gp_recv, ga_send, ga_recv,
):
    me = lax.axis_index("rows")
    right, left = lax.rem(me + 1, n), lax.rem(me + n - 1, n)
    br, slots, bs = blocks.shape[0], blocks.shape[1], blocks.shape[2]
    kv = vectors.shape[0]
    total = br * n
    first = br - HB

    def lanes(b):
        return pl.ds(pl.multiple_of(b * bs, bs), bs)

    def order(t):
        return lax.rem(t + first, br)

    def load(t):
        b = order(t)
        return pltpu.make_async_copy(blocks.at[b], stage.at[lax.rem(t, 3)], load_sem.at[lax.rem(t, 3)])

    def pload(b):
        return pltpu.make_async_copy(precond.at[b], pstage.at[lax.rem(b, 2)], pload_sem.at[lax.rem(b, 2)])

    load(0).start()
    load(1).start()
    load(2).start()
    pload(0).start()
    pload(1).start()

    barrier = pltpu.get_barrier_semaphore()

    def greet(d, _):
        pl.semaphore_signal(barrier, inc=1, device_id=(lax.rem(me + d, n),), device_id_type=MESH)
        return 0

    lax.fori_loop(1, n, greet, 0)

    def take_vectors(b, _):
        x = vectors[:, lanes(b)]
        field[b] = x
        high, low = split(x)
        pair[b, :kv] = high
        pair[b, kv:] = low
        return 0

    lax.fori_loop(0, br, take_vectors, 0)
    pair[br + HB] = jnp.zeros((2 * kv, bs), BF16)
    pl.semaphore_wait(barrier, n - 1)

    def offset(b, s):
        return lax.rem(cols[b, s] - (me * br + b) + total, total)

    def spread(b):
        moved = dot3(pair[b], w_high[b], w_low[b], NN)
        parts = [moved[:, s * bs:(s + 1) * bs] for s in range(slots)]
        offs = [jnp.where(s < counts[b], offset(b, s), HB + 1) for s in range(slots)]
        for k in range(HB + 1):
            got = acc[b + k]
            for s in range(slots):
                got = got + jnp.where(offs[s] == k, 1.0, 0.0).astype(F32) * parts[s]
            acc[b + k] = got

    def forward(b):
        picks = []
        for s in range(slots):
            at = jnp.where(s < counts[b], b + offset(b, s), br + HB)
            picks.append(pair[at])
        wide = jnp.concatenate(picks, axis=1)
        acc[b] = acc[b] + dot3(wide, w_high[b], w_low[b], NT)

    def take_tiles(t):
        load(t).wait()
        b = order(t)
        for s in range(slots):
            high, low = split(stage[lax.rem(t, 3), s])
            w_high[b, :, s * bs:(s + 1) * bs] = high
            w_low[b, :, s * bs:(s + 1) * bs] = low

        @pl.when(t + 3 < br)
        def _():
            load(t + 3).start()

    def operate(k, loading):
        halo = pltpu.make_async_remote_copy(
            src_ref=field.at[pl.ds(0, HB)], dst_ref=halo_in.at[k],
            send_sem=halo_send.at[k], recv_sem=halo_recv.at[k],
            device_id=(left,), device_id_type=MESH)
        halo.start()

        def clear(b, _):
            acc[b] = jnp.zeros((kv, bs), F32)
            return 0

        lax.fori_loop(0, br + HB, clear, 0)

        def late(t, _):
            if loading:
                take_tiles(t)
            spread(first + t)
            return 0

        lax.fori_loop(0, HB, late, 0)
        land = pltpu.make_async_remote_copy(
            src_ref=acc.at[pl.ds(br, HB)], dst_ref=land_in.at[k],
            send_sem=land_send.at[k], recv_sem=land_recv.at[k],
            device_id=(right,), device_id_type=MESH)
        land.start()

        def main(b, _):
            if loading:
                take_tiles(b + HB)
            spread(b)
            if not loading:
                forward(b)
            return 0

        lax.fori_loop(0, first, main, 0)
        if loading:
            def again(b, _):
                forward(b)
                return 0

            lax.fori_loop(0, first, again, 0)
        halo.wait_recv()

        def take_halo(i, _):
            high, low = split(halo_in[k, i])
            pair[br + i, :kv] = high
            pair[br + i, kv:] = low
            return 0

        lax.fori_loop(0, HB, take_halo, 0)

        def tail(b, _):
            forward(b)
            return 0

        lax.fori_loop(first, br, tail, 0)
        land.wait_recv()

        def take_land(i, _):
            acc[i] = acc[i] + land_in[k, i]
            return 0

        lax.fori_loop(0, HB, take_land, 0)
        halo.wait_send()
        land.wait_send()

    def sum_copy(k, d):
        return pltpu.make_async_remote_copy(
            src_ref=part.at[k], dst_ref=sums_in.at[k, me],
            send_sem=sum_send.at[k, d], recv_sem=sum_recv.at[k, me],
            device_id=(lax.rem(me + d, n),), device_id_type=MESH)

    def sum_start(k, one, two):
        folded = jnp.concatenate([one, two], axis=0)
        folded = folded[:, :128] + folded[:, 128:]
        wide = jnp.broadcast_to(jnp.sum(folded, axis=1, keepdims=True), (2 * kv, 128))
        wide = jnp.concatenate([wide, jnp.zeros((128 - 2 * kv, 128), F32)], axis=0)
        mine = wide.T[:8]
        part[k] = mine
        sums_in[k, me] = mine

        def send(d, _):
            sum_copy(k, d).start()
            return 0

        lax.fori_loop(1, n, send, 0)

    def sum_finish(k):
        def arrive(d, _):
            who = lax.rem(me + d, n)
            pltpu.make_async_remote_copy(
                src_ref=part.at[k], dst_ref=sums_in.at[k, who],
                send_sem=sum_send.at[k, d], recv_sem=sum_recv.at[k, who],
                device_id=(who,), device_id_type=MESH).wait_recv()
            return 0

        lax.fori_loop(1, n, arrive, 0)

        def add(i, so_far):
            return so_far + sums_in[k, i]

        whole = lax.fori_loop(0, n, add, jnp.zeros((8, 128), F32))

        def sent(d, _):
            sum_copy(k, d).wait_send()
            return 0

        lax.fori_loop(1, n, sent, 0)
        column = jnp.broadcast_to(whole[0:1], (128, 128)).T
        column = jnp.concatenate([column, column], axis=1)
        return column[:kv], column[kv:2 * kv]

    zero = jnp.zeros((kv, bs), F32)
    operate(0, True)

    def rayleigh(b, sums):
        x = vectors[:, lanes(b)]
        y = acc[b] + onsite[:, lanes(b)] * x
        image[b] = y
        return sums[0] + x * y, sums[1] + x * x

    sum_start(0, *lax.fori_loop(0, br, rayleigh, (zero, zero)))

    def take_precond(b, _):
        pload(b).wait()
        high, low = split(pstage[lax.rem(b, 2)])
        m_high[b] = high
        m_low[b] = low

        @pl.when(b + 2 < br)
        def _():
            pload(b + 2).start()
        correction[:, lanes(b)] = zero
        hcorr[b] = zero
        return 0

    lax.fori_loop(0, br, take_precond, 0)
    numerator, denominator = sum_finish(0)
    quotient = numerator / denominator

    def begin(b, _):
        rem[b] = quotient * vectors[:, lanes(b)] - image[b]
        return 0

    lax.fori_loop(0, br, begin, 0)

    def precondition(source):
        def body(b, _):
            high, low = split(source[b])
            x = dot3(jnp.concatenate([high, low], axis=0), m_high[b], m_low[b], NT)
            field[b] = x
            high, low = split(x)
            pair[b, :kv] = high
            pair[b, kv:] = low
            return 0

        lax.fori_loop(0, br, body, 0)

    precondition(rem)
    operate(1, False)

    def apply(b, sums):
        x = field[b]
        y = acc[b] + (onsite[:, lanes(b)] - quotient) * x
        srch[b] = x
        app[b] = y
        return sums[0] + y * rem[b], sums[1] + y * y

    sum_start(1, *lax.fori_loop(0, br, apply, (zero, zero)))
    for it in range(ITERS):
        last = it == ITERS - 1
        if not last:
            precondition(app)
            operate(it + 2, False)
        cross, own = sum_finish(it + 1)
        step = cross / (own + 1.0)

        def update(b, sums):
            x, y = srch[b], app[b]
            correction[:, lanes(b)] = correction[:, lanes(b)] + step * x
            hcorr[b] = hcorr[b] + step * (y + quotient * x)
            if last:
                return sums
            turned = field[b]
            r = rem[b] - step * y
            z = y - step * (acc[b] + (onsite[:, lanes(b)] - quotient) * turned)
            srch[b] = x - step * turned
            rem[b] = r
            app[b] = z
            return sums[0] + z * r, sums[1] + z * z

        sums = lax.fori_loop(0, br, update, (zero, zero))
        if not last:
            sum_start(it + 2, *sums)

    nb = 3 * kv

    def gram(b, so_far):
        basis = jnp.concatenate(
            [vectors[:, lanes(b)], prev_vectors[:, lanes(b)], correction[:, lanes(b)]], axis=0)
        other = jnp.concatenate([image[b], prev_image[:, lanes(b)], hcorr[b]], axis=0)
        bh, bl = split(basis)
        oh, ol = split(other)
        high = jnp.concatenate([bh, oh], axis=0)
        low = jnp.concatenate([bl, ol], axis=0)
        return so_far + dot(bh, high, NT) + dot(bl, high, NT) + dot(bh, low, NT)

    both = lax.fori_loop(0, br, gram, jnp.zeros((nb, 2 * nb), F32))
    pad = jnp.zeros((nb, 128 - nb), F32)
    sheet = jnp.concatenate(
        [jnp.concatenate([both[:, :nb], pad], axis=1), jnp.concatenate([both[:, nb:], pad], axis=1)],
        axis=0)
    chunks = 2 * nb // 8
    for c in range(chunks):
        gp[c] = sheet[c * 8:(c + 1) * 8]

    def scatter(d):
        to = lax.rem(me + d, n)
        return to, pltpu.make_async_remote_copy(
            src_ref=gp.at[jnp.minimum(to, chunks - 1)], dst_ref=gp_in.at[me],
            send_sem=gp_send.at[d], recv_sem=gp_recv.at[me],
            device_id=(to,), device_id_type=MESH)

    def scatter_send(d, _):
        to, copy = scatter(d)

        @pl.when(to < chunks)
        def _():
            copy.start()
        return 0

    lax.fori_loop(1, n, scatter_send, 0)

    def gather(d):
        to = lax.rem(me + d, n)
        return pltpu.make_async_remote_copy(
            src_ref=gsum, dst_ref=gall.at[me],
            send_sem=ga_send.at[d], recv_sem=ga_recv.at[me],
            device_id=(to,), device_id_type=MESH)

    @pl.when(me < chunks)
    def _():
        gp_in[me] = gp[me]

        def arrive(d, _):
            who = lax.rem(me + d, n)
            pltpu.make_async_remote_copy(
                src_ref=gsum, dst_ref=gp_in.at[who],
                send_sem=gp_send.at[d], recv_sem=gp_recv.at[who],
                device_id=(who,), device_id_type=MESH).wait_recv()
            return 0

        lax.fori_loop(1, n, arrive, 0)

        def add(i, so_far):
            return so_far + gp_in[i]

        mine = lax.fori_loop(0, n, add, jnp.zeros((8, 128), F32))
        gsum[...] = mine
        gall[me] = mine

        def send(d, _):
            gather(d).start()
            return 0

        lax.fori_loop(1, n, send, 0)

    def gathered(c, _):
        @pl.when(c != me)
        def _():
            pltpu.make_async_remote_copy(
                src_ref=gsum, dst_ref=gall.at[c],
                send_sem=ga_send.at[0], recv_sem=ga_recv.at[c],
                device_id=(right,), device_id_type=MESH).wait_recv()
        return 0

    lax.fori_loop(0, chunks, gathered, 0)

    def scatter_done(d, _):
        to, copy = scatter(d)

        @pl.when(to < chunks)
        def _():
            copy.wait_send()

        @pl.when(me < chunks)
        def _():
            gather(d).wait_send()
        return 0

    lax.fori_loop(1, n, scatter_done, 0)

    rows_at = lax.broadcasted_iota(jnp.int32, (nb, 128), 0)
    cols_at = lax.broadcasted_iota(jnp.int32, (nb, 128), 1)
    eye = jnp.where(rows_at == cols_at, 1.0, 0.0).astype(F32)
    half = chunks // 2
    g = jnp.concatenate([gall[c] for c in range(half)], axis=0)
    p = jnp.concatenate([gall[half + c] for c in range(half)], axis=0)
    work[:, 0:128] = g + eye
    work[:, 128:256] = p
    work[:, 256:384] = eye

    def eliminate(j, _):
        column = jnp.sum(jnp.where(cols_at == j, work[:, 0:128], 0.0), axis=1, keepdims=True)
        row = work[pl.ds(j, 1), :]
        pivot = jnp.sum(jnp.where(lax.broadcasted_iota(jnp.int32, (1, 128), 1) == j, row[:, :128], 0.0), axis=1, keepdims=True)
        root = 1.0 / jnp.sqrt(pivot)
        row = row * root
        below = jnp.where(rows_at[:, 0:1] > j, column * root, 0.0)
        work[...] = work[...] - below * row
        work[pl.ds(j, 1), :] = row
        return 0

    lax.fori_loop(0, nb, eliminate, 0)
    half_way = work[:, 128:256]
    inverse = work[:, 256:384]
    answer = lax.dot_general(
        half_way[:, :nb], inverse[:, :nb], NT, precision=lax.Precision.HIGHEST,
        preferred_element_type=F32)
    reduced[...] = answer


def local(blocks, block_cols, live_counts, onsite_energy, precond, vectors, prev_vectors, prev_image):
    n = lax.axis_size("rows")
    br, slots, bs, _ = blocks.shape
    kv, width = vectors.shape
    nb = 3 * kv
    vmem = pl.BlockSpec(memory_space=pltpu.VMEM)
    smem = pl.BlockSpec(memory_space=pltpu.SMEM)
    hbm = pl.BlockSpec(memory_space=pl.ANY)
    dma = pltpu.SemaphoreType.DMA
    rounds = ITERS + 1
    chunks = 2 * nb // 8
    return pl.pallas_call(
        functools.partial(kernel, n),
        out_shape=(
            jax.ShapeDtypeStruct((kv, width), F32),
            jax.ShapeDtypeStruct((nb, nb), F32),
        ),
        in_specs=[smem, smem, hbm, hbm, vmem, vmem, vmem, vmem],
        out_specs=(vmem, vmem),
        scratch_shapes=[
            pltpu.VMEM((br, bs, slots * bs), BF16),
            pltpu.VMEM((br, bs, slots * bs), BF16),
            pltpu.VMEM((br, bs, bs), BF16),
            pltpu.VMEM((br, bs, bs), BF16),
            pltpu.VMEM((3, slots, bs, bs), F32),
            pltpu.VMEM((2, bs, bs), F32),
            pltpu.VMEM((br, kv, bs), F32),
            pltpu.VMEM((br + HB + 1, 2 * kv, bs), BF16),
            pltpu.VMEM((br + HB, kv, bs), F32),
            pltpu.VMEM((br, kv, bs), F32),
            pltpu.VMEM((br, kv, bs), F32),
            pltpu.VMEM((br, kv, bs), F32),
            pltpu.VMEM((br, kv, bs), F32),
            pltpu.VMEM((br, kv, bs), F32),
            pltpu.VMEM((rounds, HB, kv, bs), F32),
            pltpu.VMEM((rounds, HB, kv, bs), F32),
            pltpu.VMEM((rounds, 8, 128), F32),
            pltpu.VMEM((rounds, n, 8, 128), F32),
            pltpu.VMEM((chunks, 8, 128), F32),
            pltpu.VMEM((n, 8, 128), F32),
            pltpu.VMEM((8, 128), F32),
            pltpu.VMEM((chunks, 8, 128), F32),
            pltpu.VMEM((nb, 384), F32),
            dma((3,)),
            dma((2,)),
            dma((rounds,)),
            dma((rounds,)),
            dma((rounds,)),
            dma((rounds,)),
            dma((rounds, n)),
            dma((rounds, n)),
            dma((n,)),
            dma((n,)),
            dma((n,)),
            dma((n,)),
        ],
        compiler_params=pltpu.CompilerParams(
            collective_id=0, has_side_effects=True, vmem_limit_bytes=60 * 1024 * 1024
        ),
    )(block_cols, live_counts, blocks, precond, onsite_energy[None, :], vectors, prev_vectors, prev_image)


def solution(mesh):
    placed = (
        P("rows", None, None, None),
        P("rows", None),
        P("rows"),
        P("rows"),
        P("rows", None, None),
        P(None, "rows"),
        P(None, "rows"),
        P(None, "rows"),
    )
    return jax.shard_map(
        local, mesh=mesh, in_specs=placed, out_specs=(P(None, "rows"), P()), check_vma=False
    )
```

```python
import functools

import jax
import jax.numpy as jnp
from jax import lax
from jax.experimental import pallas as pl
from jax.experimental.pallas import tpu as pltpu
from jax.sharding import PartitionSpec as P

HB = 4
ITERS = 3
MESH = pl.DeviceIdType.MESH
F32 = jnp.float32
BF16 = jnp.bfloat16
NN = (((1,), (0,)), ((), ()))
NT = (((1,), (1,)), ((), ()))


def split(x):
    high = x.astype(BF16)
    low = (x - high.astype(F32)).astype(BF16)
    return high, low


def dot(a, b, dims):
    return lax.dot_general(a, b, dims, preferred_element_type=F32)


def dot3(pair, high, low, dims):
    rows = pair.shape[0] // 2
    both = dot(pair, high, dims)
    return both[:rows] + both[rows:] + dot(pair[:rows], low, dims)


def kernel(
    n, cols, counts, blocks, precond, onsite, vectors, prev_vectors, prev_image,
    correction, reduced,
    w_high, w_low, m_high, m_low, stage, pstage, field, pair, acc, image, rem, app, hcorr, srch,
    halo_in, land_in, part, sums_in, gp, gp_in, gsum, gall, work,
    load_sem, pload_sem, halo_send, halo_recv, land_send, land_recv,
    sum_send, sum_recv, gp_send, gp_recv, ga_send, ga_recv,
):
    me = lax.axis_index("rows")
    right, left = lax.rem(me + 1, n), lax.rem(me + n - 1, n)
    br, slots, bs = blocks.shape[0], blocks.shape[1], blocks.shape[2]
    kv = vectors.shape[0]
    total = br * n
    first = br - HB

    def lanes(b):
        return pl.ds(pl.multiple_of(b * bs, bs), bs)

    def order(t):
        return lax.rem(t + first, br)

    def load(t):
        b = order(t)
        return pltpu.make_async_copy(blocks.at[b], stage.at[lax.rem(t, 3)], load_sem.at[lax.rem(t, 3)])

    def pload(b):
        return pltpu.make_async_copy(precond.at[b], pstage.at[lax.rem(b, 2)], pload_sem.at[lax.rem(b, 2)])

    load(0).start()
    load(1).start()
    load(2).start()
    pload(0).start()
    pload(1).start()

    barrier = pltpu.get_barrier_semaphore()

    def greet(d, _):
        pl.semaphore_signal(barrier, inc=1, device_id=(lax.rem(me + d, n),), device_id_type=MESH)
        return 0

    lax.fori_loop(1, n, greet, 0)

    def take_vectors(b, _):
        x = vectors[:, lanes(b)]
        field[b] = x
        high, low = split(x)
        pair[b, :kv] = high
        pair[b, kv:] = low
        return 0

    lax.fori_loop(0, br, take_vectors, 0)
    pair[br + HB] = jnp.zeros((2 * kv, bs), BF16)
    pl.semaphore_wait(barrier, n - 1)

    def offset(b, s):
        return lax.rem(cols[b, s] - (me * br + b) + total, total)

    def spread(b):
        moved = dot3(pair[b], w_high[b], w_low[b], NN)
        parts = [moved[:, s * bs:(s + 1) * bs] for s in range(slots)]
        offs = [jnp.where(s < counts[b], offset(b, s), HB + 1) for s in range(slots)]
        for k in range(HB + 1):
            got = acc[b + k]
            for s in range(slots):
                got = got + jnp.where(offs[s] == k, 1.0, 0.0).astype(F32) * parts[s]
            acc[b + k] = got

    def forward(b):
        picks = []
        for s in range(slots):
            at = jnp.where(s < counts[b], b + offset(b, s), br + HB)
            picks.append(pair[at])
        wide = jnp.concatenate(picks, axis=1)
        acc[b] = acc[b] + dot3(wide, w_high[b], w_low[b], NT)

    def take_tiles(t):
        load(t).wait()
        b = order(t)
        for s in range(slots):
            high, low = split(stage[lax.rem(t, 3), s])
            w_high[b, :, s * bs:(s + 1) * bs] = high
            w_low[b, :, s * bs:(s + 1) * bs] = low

        @pl.when(t + 3 < br)
        def _():
            load(t + 3).start()

    def operate(k, loading):
        halo = pltpu.make_async_remote_copy(
            src_ref=field.at[pl.ds(0, HB)], dst_ref=halo_in.at[k],
            send_sem=halo_send.at[k], recv_sem=halo_recv.at[k],
            device_id=(left,), device_id_type=MESH)
        halo.start()

        def clear(b, _):
            acc[b] = jnp.zeros((kv, bs), F32)
            return 0

        lax.fori_loop(0, br + HB, clear, 0)

        def late(t, _):
            if loading:
                take_tiles(t)
            spread(first + t)
            return 0

        lax.fori_loop(0, HB, late, 0, unroll=1 if loading else 2)
        land = pltpu.make_async_remote_copy(
            src_ref=acc.at[pl.ds(br, HB)], dst_ref=land_in.at[k],
            send_sem=land_send.at[k], recv_sem=land_recv.at[k],
            device_id=(right,), device_id_type=MESH)
        land.start()

        def main(b, _):
            if loading:
                take_tiles(b + HB)
            spread(b)
            if not loading:
                forward(b)
            return 0

        lax.fori_loop(0, first, main, 0, unroll=1 if loading else 2)
        if loading:
            def again(b, _):
                forward(b)
                return 0

            lax.fori_loop(0, first, again, 0, unroll=2)
        halo.wait_recv()

        def take_halo(i, _):
            high, low = split(halo_in[k, i])
            pair[br + i, :kv] = high
            pair[br + i, kv:] = low
            return 0

        lax.fori_loop(0, HB, take_halo, 0)

        def tail(b, _):
            forward(b)
            return 0

        lax.fori_loop(first, br, tail, 0, unroll=2)
        land.wait_recv()

        def take_land(i, _):
            acc[i] = acc[i] + land_in[k, i]
            return 0

        lax.fori_loop(0, HB, take_land, 0)
        halo.wait_send()
        land.wait_send()

    def sum_copy(k, d):
        return pltpu.make_async_remote_copy(
            src_ref=part.at[k], dst_ref=sums_in.at[k, me],
            send_sem=sum_send.at[k, d], recv_sem=sum_recv.at[k, me],
            device_id=(lax.rem(me + d, n),), device_id_type=MESH)

    def sum_start(k, one, two):
        folded = jnp.concatenate([one, two], axis=0)
        folded = folded[:, :128] + folded[:, 128:]
        wide = jnp.broadcast_to(jnp.sum(folded, axis=1, keepdims=True), (2 * kv, 128))
        wide = jnp.concatenate([wide, jnp.zeros((128 - 2 * kv, 128), F32)], axis=0)
        mine = wide.T[:8]
        part[k] = mine
        sums_in[k, me] = mine

        def send(d, _):
            sum_copy(k, d).start()
            return 0

        lax.fori_loop(1, n, send, 0)

    def sum_finish(k):
        def arrive(d, _):
            who = lax.rem(me + d, n)
            pltpu.make_async_remote_copy(
                src_ref=part.at[k], dst_ref=sums_in.at[k, who],
                send_sem=sum_send.at[k, d], recv_sem=sum_recv.at[k, who],
                device_id=(who,), device_id_type=MESH).wait_recv()
            return 0

        lax.fori_loop(1, n, arrive, 0)

        def add(i, so_far):
            return so_far + sums_in[k, i]

        whole = lax.fori_loop(0, n, add, jnp.zeros((8, 128), F32))

        def sent(d, _):
            sum_copy(k, d).wait_send()
            return 0

        lax.fori_loop(1, n, sent, 0)
        column = jnp.broadcast_to(whole[0:1], (128, 128)).T
        column = jnp.concatenate([column, column], axis=1)
        return column[:kv], column[kv:2 * kv]

    zero = jnp.zeros((kv, bs), F32)
    operate(0, True)

    def rayleigh(b, sums):
        x = vectors[:, lanes(b)]
        y = acc[b] + onsite[:, lanes(b)] * x
        image[b] = y
        return sums[0] + x * y, sums[1] + x * x

    sum_start(0, *lax.fori_loop(0, br, rayleigh, (zero, zero)))

    def take_precond(b, _):
        pload(b).wait()
        high, low = split(pstage[lax.rem(b, 2)])
        m_high[b] = high
        m_low[b] = low

        @pl.when(b + 2 < br)
        def _():
            pload(b + 2).start()
        correction[:, lanes(b)] = zero
        hcorr[b] = zero
        return 0

    lax.fori_loop(0, br, take_precond, 0)
    numerator, denominator = sum_finish(0)
    quotient = numerator / denominator

    def begin(b, _):
        rem[b] = quotient * vectors[:, lanes(b)] - image[b]
        return 0

    lax.fori_loop(0, br, begin, 0)

    def precondition(source):
        def body(b, _):
            high, low = split(source[b])
            x = dot3(jnp.concatenate([high, low], axis=0), m_high[b], m_low[b], NT)
            field[b] = x
            high, low = split(x)
            pair[b, :kv] = high
            pair[b, kv:] = low
            return 0

        lax.fori_loop(0, br, body, 0, unroll=4)

    precondition(rem)
    operate(1, False)

    def apply(b, sums):
        x = field[b]
        y = acc[b] + (onsite[:, lanes(b)] - quotient) * x
        srch[b] = x
        app[b] = y
        return sums[0] + y * rem[b], sums[1] + y * y

    sum_start(1, *lax.fori_loop(0, br, apply, (zero, zero)))
    for it in range(ITERS):
        last = it == ITERS - 1
        if not last:
            precondition(app)
            operate(it + 2, False)
        cross, own = sum_finish(it + 1)
        step = cross / (own + 1.0)

        def update(b, sums):
            x, y = srch[b], app[b]
            correction[:, lanes(b)] = correction[:, lanes(b)] + step * x
            hcorr[b] = hcorr[b] + step * (y + quotient * x)
            if last:
                return sums
            turned = field[b]
            r = rem[b] - step * y
            z = y - step * (acc[b] + (onsite[:, lanes(b)] - quotient) * turned)
            srch[b] = x - step * turned
            rem[b] = r
            app[b] = z
            return sums[0] + z * r, sums[1] + z * z

        sums = lax.fori_loop(0, br, update, (zero, zero), unroll=2)
        if not last:
            sum_start(it + 2, *sums)

    nb = 3 * kv

    def gram(b, so_far):
        basis = jnp.concatenate(
            [vectors[:, lanes(b)], prev_vectors[:, lanes(b)], correction[:, lanes(b)]], axis=0)
        other = jnp.concatenate([image[b], prev_image[:, lanes(b)], hcorr[b]], axis=0)
        bh, bl = split(basis)
        oh, ol = split(other)
        high = jnp.concatenate([bh, oh], axis=0)
        low = jnp.concatenate([bl, ol], axis=0)
        return so_far + dot(bh, high, NT) + dot(bl, high, NT) + dot(bh, low, NT)

    both = lax.fori_loop(0, br, gram, jnp.zeros((nb, 2 * nb), F32), unroll=2)
    pad = jnp.zeros((nb, 128 - nb), F32)
    sheet = jnp.concatenate(
        [jnp.concatenate([both[:, :nb], pad], axis=1), jnp.concatenate([both[:, nb:], pad], axis=1)],
        axis=0)
    chunks = 2 * nb // 8
    for c in range(chunks):
        gp[c] = sheet[c * 8:(c + 1) * 8]

    def scatter(d):
        to = lax.rem(me + d, n)
        return to, pltpu.make_async_remote_copy(
            src_ref=gp.at[jnp.minimum(to, chunks - 1)], dst_ref=gp_in.at[me],
            send_sem=gp_send.at[d], recv_sem=gp_recv.at[me],
            device_id=(to,), device_id_type=MESH)

    def scatter_send(d, _):
        to, copy = scatter(d)

        @pl.when(to < chunks)
        def _():
            copy.start()
        return 0

    lax.fori_loop(1, n, scatter_send, 0)

    def gather(d):
        to = lax.rem(me + d, n)
        return pltpu.make_async_remote_copy(
            src_ref=gsum, dst_ref=gall.at[me],
            send_sem=ga_send.at[d], recv_sem=ga_recv.at[me],
            device_id=(to,), device_id_type=MESH)

    @pl.when(me < chunks)
    def _():
        gp_in[me] = gp[me]

        def arrive(d, _):
            who = lax.rem(me + d, n)
            pltpu.make_async_remote_copy(
                src_ref=gsum, dst_ref=gp_in.at[who],
                send_sem=gp_send.at[d], recv_sem=gp_recv.at[who],
                device_id=(who,), device_id_type=MESH).wait_recv()
            return 0

        lax.fori_loop(1, n, arrive, 0)

        def add(i, so_far):
            return so_far + gp_in[i]

        mine = lax.fori_loop(0, n, add, jnp.zeros((8, 128), F32))
        gsum[...] = mine
        gall[me] = mine

        def send(d, _):
            gather(d).start()
            return 0

        lax.fori_loop(1, n, send, 0)

    def gathered(c, _):
        @pl.when(c != me)
        def _():
            pltpu.make_async_remote_copy(
                src_ref=gsum, dst_ref=gall.at[c],
                send_sem=ga_send.at[0], recv_sem=ga_recv.at[c],
                device_id=(right,), device_id_type=MESH).wait_recv()
        return 0

    lax.fori_loop(0, chunks, gathered, 0)

    def scatter_done(d, _):
        to, copy = scatter(d)

        @pl.when(to < chunks)
        def _():
            copy.wait_send()

        @pl.when(me < chunks)
        def _():
            gather(d).wait_send()
        return 0

    lax.fori_loop(1, n, scatter_done, 0)

    rows_at = lax.broadcasted_iota(jnp.int32, (nb, 128), 0)
    cols_at = lax.broadcasted_iota(jnp.int32, (nb, 128), 1)
    eye = jnp.where(rows_at == cols_at, 1.0, 0.0).astype(F32)
    half = chunks // 2
    g = jnp.concatenate([gall[c] for c in range(half)], axis=0)
    p = jnp.concatenate([gall[half + c] for c in range(half)], axis=0)
    work[:, 0:128] = g + eye
    work[:, 128:256] = p
    work[:, 256:384] = eye

    def eliminate(j, _):
        column = jnp.sum(jnp.where(cols_at == j, work[:, 0:128], 0.0), axis=1, keepdims=True)
        row = work[pl.ds(j, 1), :]
        pivot = jnp.sum(jnp.where(lane_at == j, row[:, :128], 0.0), axis=1, keepdims=True)
        below = jnp.where(rows_at[:, 0:1] > j, column / pivot, 0.0)
        work[...] = work[...] - below * row
        return 0

    lane_at = lax.broadcasted_iota(jnp.int32, (1, 128), 1)
    lax.fori_loop(0, nb, eliminate, 0, unroll=2)
    diagonal = jnp.sum(jnp.where(rows_at == cols_at, work[:, 0:128], 0.0), axis=1, keepdims=True)
    scale = 1.0 / jnp.sqrt(diagonal)
    half_way = scale * work[:, 128:256]
    inverse = scale * work[:, 256:384]
    answer = lax.dot_general(
        half_way[:, :nb], inverse[:, :nb], NT, precision=lax.Precision.HIGHEST,
        preferred_element_type=F32)
    reduced[...] = answer


def local(blocks, block_cols, live_counts, onsite_energy, precond, vectors, prev_vectors, prev_image):
    n = lax.axis_size("rows")
    br, slots, bs, _ = blocks.shape
    kv, width = vectors.shape
    nb = 3 * kv
    vmem = pl.BlockSpec(memory_space=pltpu.VMEM)
    smem = pl.BlockSpec(memory_space=pltpu.SMEM)
    hbm = pl.BlockSpec(memory_space=pl.ANY)
    dma = pltpu.SemaphoreType.DMA
    rounds = ITERS + 1
    chunks = 2 * nb // 8
    return pl.pallas_call(
        functools.partial(kernel, n),
        out_shape=(
            jax.ShapeDtypeStruct((kv, width), F32),
            jax.ShapeDtypeStruct((nb, nb), F32),
        ),
        in_specs=[smem, smem, hbm, hbm, vmem, vmem, vmem, vmem],
        out_specs=(vmem, vmem),
        scratch_shapes=[
            pltpu.VMEM((br, bs, slots * bs), BF16),
            pltpu.VMEM((br, bs, slots * bs), BF16),
            pltpu.VMEM((br, bs, bs), BF16),
            pltpu.VMEM((br, bs, bs), BF16),
            pltpu.VMEM((3, slots, bs, bs), F32),
            pltpu.VMEM((2, bs, bs), F32),
            pltpu.VMEM((br, kv, bs), F32),
            pltpu.VMEM((br + HB + 1, 2 * kv, bs), BF16),
            pltpu.VMEM((br + HB, kv, bs), F32),
            pltpu.VMEM((br, kv, bs), F32),
            pltpu.VMEM((br, kv, bs), F32),
            pltpu.VMEM((br, kv, bs), F32),
            pltpu.VMEM((br, kv, bs), F32),
            pltpu.VMEM((br, kv, bs), F32),
            pltpu.VMEM((rounds, HB, kv, bs), F32),
            pltpu.VMEM((rounds, HB, kv, bs), F32),
            pltpu.VMEM((rounds, 8, 128), F32),
            pltpu.VMEM((rounds, n, 8, 128), F32),
            pltpu.VMEM((chunks, 8, 128), F32),
            pltpu.VMEM((n, 8, 128), F32),
            pltpu.VMEM((8, 128), F32),
            pltpu.VMEM((chunks, 8, 128), F32),
            pltpu.VMEM((nb, 384), F32),
            dma((3,)),
            dma((2,)),
            dma((rounds,)),
            dma((rounds,)),
            dma((rounds,)),
            dma((rounds,)),
            dma((rounds, n)),
            dma((rounds, n)),
            dma((n,)),
            dma((n,)),
            dma((n,)),
            dma((n,)),
        ],
        compiler_params=pltpu.CompilerParams(
            collective_id=0, has_side_effects=True, vmem_limit_bytes=60 * 1024 * 1024
        ),
    )(block_cols, live_counts, blocks, precond, onsite_energy[None, :], vectors, prev_vectors, prev_image)


def solution(mesh):
    placed = (
        P("rows", None, None, None),
        P("rows", None),
        P("rows"),
        P("rows"),
        P("rows", None, None),
        P(None, "rows"),
        P(None, "rows"),
        P(None, "rows"),
    )
    return jax.shard_map(
        local, mesh=mesh, in_specs=placed, out_specs=(P(None, "rows"), P()), check_vma=False
    )
```
